32 devices in a mesh: rep: 4 (over x, y), dp: 8 (over z, core).
Axes of the slice: x: 2, y: 2, z: 4, core: 2. Of those that a mesh axis runs over, the one named last changes fastest.
Arguments:
- x: bfloat16 [32, 4096, 512], P(('rep', 'dp')), parts along dimension 0
- dy: bfloat16 [32, 4096, 512], P(('rep', 'dp')), parts along dimension 0
- w_gate: bfloat16 [2, 512, 1408], P(None, 'dp')
- w_up: bfloat16 [2, 512, 1408], P(None, 'dp')
- w_down: bfloat16 [2, 1408, 512], P(None, 'dp')
- m_w_gate: float32 [2, 512, 1408], P(None, 'dp')
- m_w_up: float32 [2, 512, 1408], P(None, 'dp')
- m_w_down: float32 [2, 1408, 512], P(None, 'dp')
- v_w_gate: float32 [2, 512, 1408], P(None, 'dp')
- v_w_up: float32 [2, 512, 1408], P(None, 'dp')
- v_w_down: float32 [2, 1408, 512], P(None, 'dp')
Outputs:
- output 1: bfloat16 [8, 512, 1408], P('rep', 'dp'), parts along dimension 0
- output 2: bfloat16 [8, 512, 1408], P('rep', 'dp'), parts along dimension 0
- output 3: bfloat16 [8, 1408, 512], P('rep', 'dp'), parts along dimension 0
- output 4: float32 [8, 512, 1408], P('rep', 'dp'), parts along dimension 0
- output 5: float32 [8, 512, 1408], P('rep', 'dp'), parts along dimension 0
- output 6: float32 [8, 1408, 512], P('rep', 'dp'), parts along dimension 0
- output 7: float32 [8, 512, 1408], P('rep', 'dp'), parts along dimension 0
- output 8: float32 [8, 512, 1408], P('rep', 'dp'), parts along dimension 0
- output 9: float32 [8, 1408, 512], P('rep', 'dp'), parts along dimension 0
There are 4 independent parts. The reference program is written for one: setup_inputs(seed, part) draws one part's arguments, and reference() takes and returns one part's arrays. A program takes and returns all parts, laid end to end along the dimension named above; an argument that names none is the same for every part.
All inputs are finite; a program needn't handle non-finite values.
Results may differ from the reference program's by a relative error of at most 0.022.
Values are sent between devices in bfloat16 or wider.
A program may use at most 2 GiB of HBM per device.

```python
import jax
import jax.numpy as jnp
from jax import lax

SEQUENCES = 8
TOKENS = 4096
D = 512
FF = 1408
LAYERS = 2
NAMES = ("w_gate", "w_up", "w_down")
SHAPES = {"w_gate": (LAYERS, D, FF), "w_up": (LAYERS, D, FF), "w_down": (LAYERS, FF, D)}


def bump(key, n, height):
    away = (jnp.arange(n, dtype=jnp.int32) - jax.random.randint(key, (), 0, n, jnp.int32)) % n
    return jnp.where(away < n // 8, height, 1.0)


def together(key, own, strength):
    shared = jax.random.normal(key, own.shape[1:], jnp.float32)
    return (own + strength * shared) * lax.rsqrt(1 + strength * strength)


def setup_inputs(seed: int = 0, part: int = 0) -> dict:
    kx, kdy, ka, kb, kz, kf, kh, kl, *keys = jax.random.split(jax.random.key(seed), 8 + 3 * len(NAMES))
    kx, kdy, ka, kb = (jax.random.fold_in(k, part) for k in (kx, kdy, ka, kb))
    kw, km, kv = (keys[i::3] for i in range(3))
    shape = (SEQUENCES, TOKENS, D)
    much_x, much_dy = jax.random.uniform(kz, (2,), jnp.float32, 0.0, 1.0)
    loud = 2.0 ** jax.random.uniform(jax.random.fold_in(kz, 1), (), jnp.float32, -1.0, 2.0)
    layers = 2.0 ** jax.random.uniform(kl, (LAYERS, 1, 1), jnp.float32, -1.0, 1.0)
    x = together(ka, jax.random.normal(kx, shape, jnp.float32), much_x) * bump(kf, D, 4.0)
    dy = together(kb, jax.random.normal(kdy, shape, jnp.float32), much_dy)
    drawn = {"x": x.astype(jnp.bfloat16), "dy": (loud * dy * (SEQUENCES * TOKENS) ** -0.5).astype(jnp.bfloat16)}
    for key, name in zip(kw, NAMES, strict=True):
        w = jax.random.normal(key, SHAPES[name], jnp.float32) * SHAPES[name][1] ** -0.5
        drawn[name] = (w * {"w_gate": 1.0, "w_up": bump(kh, FF, 4.0), "w_down": layers}[name]).astype(jnp.bfloat16)
    for key, name in zip(km, NAMES, strict=True):
        drawn[f"m_{name}"] = 0.1 * jax.random.normal(key, SHAPES[name], jnp.float32)
    for key, name in zip(kv, NAMES, strict=True):
        drawn[f"v_{name}"] = jax.random.uniform(key, SHAPES[name], jnp.float32, 0.005, 0.015)
    return drawn


def matmul(a, w):
    return jnp.dot(a, w, preferred_element_type=jnp.float32).astype(jnp.bfloat16)


def normed(h):
    wide = h.astype(jnp.float32)
    scale = lax.rsqrt(jnp.mean(wide**2, -1, keepdims=True) + 1e-6)
    return (wide * scale).astype(jnp.bfloat16)


def layer(h, w):
    a = normed(h)
    gate = jnp.dot(a, w["w_gate"], preferred_element_type=jnp.float32)
    up = jnp.dot(a, w["w_up"], preferred_element_type=jnp.float32)
    return h + matmul((jax.nn.silu(gate) * up).astype(jnp.bfloat16), w["w_down"])


def adamw(w, m, v, g):
    m = 0.9 * m + 0.1 * g
    v = 0.95 * v + 0.05 * g * g
    step = m * lax.rsqrt(v + 1e-8) + 0.1 * w
    return (w - 0.02 * step).astype(jnp.bfloat16), m, v


def clipped(gradients, sum_of_squares, count):
    factor = jnp.minimum(1.0, 0.5 * lax.rsqrt(sum_of_squares / count + 1e-30))
    return [g * factor for g in gradients]


def stack(weights, h):
    return lax.scan(lambda h, w: (layer(h, w), None), h, weights)[0]


def reference(x, dy, w_gate, w_up, w_down, m_w_gate, m_w_up, m_w_down, v_w_gate, v_w_up, v_w_down):
    weights = dict(zip(NAMES, (w_gate, w_up, w_down), strict=True))

    def take(so_far, sequence):
        h, by_y = sequence
        _, back = jax.vjp(lambda w: stack(w, h), weights)
        return jax.tree.map(lambda total, term: total + term.astype(jnp.float32), so_far, back(by_y)[0]), None

    none_yet = {name: jnp.zeros(w.shape, jnp.float32) for name, w in weights.items()}
    by_weights, _ = lax.scan(take, none_yet, (x, dy))
    gradients = [by_weights[name].astype(jnp.bfloat16).astype(jnp.float32) for name in NAMES]
    gradients = clipped(gradients, sum(jnp.sum(g * g) for g in gradients), sum(g.size for g in gradients))
    new = [
        adamw(w.astype(jnp.float32), m, v, g)
        for w, m, v, g in zip((w_gate, w_up, w_down), (m_w_gate, m_w_up, m_w_down), (v_w_gate, v_w_up, v_w_down), gradients, strict=True)
    ]
    return tuple(one[which] for which in range(3) for one in new)
```

```python
import functools

import jax
import jax.numpy as jnp
from jax import lax
from jax.experimental import pallas as pl
from jax.experimental.pallas import tpu as pltpu
from jax.sharding import PartitionSpec as P

MESH = pl.DeviceIdType.MESH
F32, BF16 = jnp.float32, jnp.bfloat16
T, D, FF = 4096, 512, 1408
DEV = 8
C = 256
NK = 6
NJ = 2 * NK
SH = C // DEV
ROWS = 192
TB = 512
NT = T // TB


def normed(wide):
    scale = lax.rsqrt(jnp.mean(wide * wide, -1, keepdims=True) + 1e-6)
    return (wide * scale).astype(BF16)


def dot(a, b):
    return jnp.dot(a, b, preferred_element_type=F32)


def kernel(
    x_hbm, dy_hbm, p_hbm, g_out, sq_out,
    wbuf, a0, a1, at, by, byt, h1, acc, wgu, wd, wdt, wt, gd, ggu, pg, rx, tx, rl, rz, sq, nb,
    local_sem, s1_send, s1_recv, s2_send, s2_recv, s3_send, s3_recv,
    d_send, d_recv, z_send, z_recv, r_recv, n_send, n_recv,
):
    rep, dp = lax.axis_index("rep"), lax.axis_index("dp")
    z, c = dp // 2, dp % 2
    partner = z * 2 + (1 - c)
    outer = (z == 0) | (z == 3)
    inner = (z == 1) | (z == 2)
    near, far, opposite = 1 + z // 3, 2 - z // 3, 3 - z
    other_outer = 3 * (z - 1)
    other_outer = jnp.where(inner, other_outer, 0)
    far_outer = 3 - other_outer

    copies = [
        pltpu.make_async_copy(p_hbm, wbuf.at[:, c, z], local_sem.at[0]),
        pltpu.make_async_copy(x_hbm, h1, local_sem.at[1]),
        pltpu.make_async_copy(dy_hbm, by, local_sem.at[2]),
    ]
    for copy in copies:
        copy.start()
    barrier = pltpu.get_barrier_semaphore()
    for i in range(1, DEV):
        pl.semaphore_signal(barrier, inc=1, device_id=(rep, (dp + i) % DEV), device_id_type=MESH)
    for i in range(1, 4):
        pl.semaphore_signal(barrier, inc=1, device_id=((rep + i) % 4, dp), device_id_type=MESH)
    pl.semaphore_wait(barrier, DEV - 1 + 3)

    def quarter(j, zz, rr):
        return wbuf.at[j, c, zz, pl.ds(pl.multiple_of(rr * (ROWS // 4), 16), ROWS // 4)]

    def along_z(j, i):
        ref = quarter(j, z, rep)
        return pltpu.make_async_remote_copy(
            src_ref=ref, dst_ref=ref, send_sem=s1_send.at[j, i - 1], recv_sem=s1_recv.at[j, i - 1],
            device_id=(rep, ((z + i) % 4) * 2 + c), device_id_type=MESH)

    def from_z(j, i):
        ref = quarter(j, (z + 4 - i) % 4, rep)
        return pltpu.make_async_remote_copy(
            src_ref=ref, dst_ref=ref, send_sem=s1_send.at[j, i - 1], recv_sem=s1_recv.at[j, i - 1],
            device_id=(rep, dp), device_id_type=MESH)

    def across(j, i, q):
        ref = quarter(j, (z + 4 - i) % 4, rep)
        return pltpu.make_async_remote_copy(
            src_ref=ref, dst_ref=ref, send_sem=s2_send.at[j, i - 1, q - 1], recv_sem=s2_recv.at[j, i - 1, q - 1],
            device_id=((rep + q) % 4, dp), device_id_type=MESH)

    def from_across(j, i, q):
        ref = quarter(j, (z + 4 - i) % 4, (rep + 4 - q) % 4)
        return pltpu.make_async_remote_copy(
            src_ref=ref, dst_ref=ref, send_sem=s2_send.at[j, i - 1, q - 1], recv_sem=s2_recv.at[j, i - 1, q - 1],
            device_id=(rep, dp), device_id_type=MESH)

    def to_partner(j):
        ref = wbuf.at[j, c]
        return pltpu.make_async_remote_copy(
            src_ref=ref, dst_ref=ref, send_sem=s3_send.at[j], recv_sem=s3_recv.at[j],
            device_id=(rep, partner), device_id_type=MESH)

    def from_partner(j):
        ref = wbuf.at[j, 1 - c]
        return pltpu.make_async_remote_copy(
            src_ref=ref, dst_ref=ref, send_sem=s3_send.at[j], recv_sem=s3_recv.at[j],
            device_id=(rep, dp), device_id_type=MESH)

    def stage_one(j):
        for i in (1, 2, 3):
            along_z(j, i).start()

    def stage_two(j):
        for i in (1, 2, 3):
            from_z(j, i).wait_recv()
            for q in (1, 2, 3):
                across(j, i, q).start()

    def stage_three(j):
        for i in (1, 2, 3):
            for q in (1, 2, 3):
                from_across(j, i, q).wait_recv()
        to_partner(j).start()

    copies[0].wait()
    lax.fori_loop(0, NJ, lambda j, _: (stage_one(j), 0)[1], 0)

    def exchange(q):
        return pltpu.make_async_remote_copy(
            src_ref=pg.at[q % 2, 1 - c], dst_ref=rx.at[q], send_sem=d_send.at[q], recv_sem=d_recv.at[q],
            device_id=(rep, partner), device_id_type=MESH)

    def z_copy(q, block, dst, recv_sem, n, zz):
        return pltpu.make_async_remote_copy(
            src_ref=tx.at[q % 2, block], dst_ref=dst, send_sem=z_send.at[q, n], recv_sem=recv_sem,
            device_id=(rep, zz * 2 + c), device_id_type=MESH)

    def chip_sum(q, block):
        return pg[q % 2, c, block].astype(F32) + rx[q, block].astype(F32)

    def wait_z_sends(q):
        for n in range(3):
            z_copy(q, 0, rz.at[q, 0], z_recv.at[q, 0], n, z).wait_send()

    def rs_chip(q):
        exchange(q).wait_recv()

        @pl.when(q >= 2)
        def _():
            wait_z_sends(q - 2)

        for block in range(4):
            tx[q % 2, block] = chip_sum(q, block).astype(BF16)

        @pl.when(outer)
        def _():
            z_copy(q, opposite, rl.at[q], r_recv.at[q], 0, near).start()
            z_copy(q, far, rz.at[q, 1], z_recv.at[q, 1], 1, far).start()
            z_copy(q, near, rz.at[q, 0], z_recv.at[q, 0], 2, near).start()

        @pl.when(inner)
        def _():
            z_copy(q, opposite, rz.at[q, 2], z_recv.at[q, 2], 0, opposite).start()
            z_copy(q, other_outer, rz.at[q, 0], z_recv.at[q, 0], 1, other_outer).start()

    def rs_relay(q):
        @pl.when(inner)
        def _():
            z_copy(q, 0, rl.at[q], r_recv.at[q], 2, z).wait_recv()
            tx[q % 2, far_outer] = (chip_sum(q, far_outer) + rl[q].astype(F32)).astype(BF16)
            z_copy(q, far_outer, rz.at[q, 1], z_recv.at[q, 1], 2, far_outer).start()

    def rs_final(q):
        for n in range(2):
            z_copy(q, 0, rz.at[q, n], z_recv.at[q, n], 0, z).wait_recv()
        total = chip_sum(q, z) + rz[q, 0].astype(F32) + rz[q, 1].astype(F32)

        def finish(value):
            rounded = value.astype(BF16)
            g_out[q] = rounded
            wide = rounded.astype(F32)
            sq[...] += jnp.sum((wide * wide).reshape(ROWS // 8, 8, C), 0)

        @pl.when(outer)
        def _():
            finish(total)

        @pl.when(inner)
        def _():
            z_copy(q, 0, rz.at[q, 2], z_recv.at[q, 2], 0, z).wait_recv()
            finish(total + rz[q, 2].astype(F32))

    def rs_hooks(q, t):
        @pl.when((t == 1) & (q >= 1))
        def _():
            rs_chip(q - 1)

        @pl.when((t == 4) & (q >= 1))
        def _():
            rs_relay(q - 1)

        @pl.when((t == 6) & (q >= 2))
        def _():
            rs_final(q - 2)

    def rs_begin(q):
        @pl.when(q >= 2)
        def _():
            exchange(q - 2).wait_send()

        for d in range(DEV):
            rows = slice(d * 64, d * 64 + 64)
            pg[q % 2, d % 2, d // 2, 0:64] = ggu[rows, 0:C].astype(BF16)
            pg[q % 2, d % 2, d // 2, 64:128] = ggu[rows, C : 2 * C].astype(BF16)
        turned = gd[...].astype(BF16).T
        for d in range(DEV):
            rows = slice(d * SH, d * SH + SH)
            pg[q % 2, d % 2, d // 2, 128:160] = turned[rows, 0:256]
            pg[q % 2, d % 2, d // 2, 160:192] = turned[rows, 256:512]
        exchange(q).start()

    def prepare(j, forward, input_gradient):
        for d in range(DEV):
            share = wbuf[j, d % 2, d // 2]
            wgu[d * 64 : d * 64 + 64, 0:C] = share[0:64]
            wgu[d * 64 : d * 64 + 64, C : 2 * C] = share[64:128]
            wd[d * SH : d * SH + SH, 0:256] = share[128:160]
            wd[d * SH : d * SH + SH, 256:512] = share[160:192]
        if not forward:
            wdt[...] = wd[...].T
        if input_gradient:
            wt[...] = wgu[...].T

    def tokens(t):
        return pl.ds(pl.multiple_of(t * TB, TB), TB)

    def ag_hooks(j, t):
        @pl.when((t == 1) & (j + 3 < NJ))
        def _():
            stage_two(j + 3)

        @pl.when((t == 4) & (j + 1 < NJ))
        def _():
            stage_three(j + 1)

    sq[...] = jnp.zeros_like(sq)
    copies[1].wait()
    copies[2].wait()

    def first(t, _):
        ts = tokens(t)
        a0[ts] = normed(h1[ts].astype(F32))
        byt[:, ts] = by[ts].T

        @pl.when(t >= NT - 3)
        def _():
            stage_two(t - (NT - 3))

        return 0

    lax.fori_loop(0, NT, first, 0)
    stage_three(0)

    def forward_chunk(k, _):
        from_partner(k).wait_recv()
        prepare(k, True, False)

        def step(t, _):
            ag_hooks(k, t)
            ts = tokens(t)
            gu = dot(a0[ts], wgu[...])
            gate, up = gu[:, :C], gu[:, C:]
            hidden = (gate / (1.0 + jnp.exp(-gate)) * up).astype(BF16)
            part = dot(hidden, wd[...])

            @pl.when(k == 0)
            def _():
                acc[ts] = part

            @pl.when(k != 0)
            def _():
                acc[ts] += part

            return 0

        lax.fori_loop(0, NT, step, 0)
        return 0

    lax.fori_loop(0, NK, forward_chunk, 0)

    def middle(t, _):
        ts = tokens(t)
        h = (h1[ts].astype(F32) + acc[ts].astype(BF16).astype(F32)).astype(BF16)
        h1[ts] = h
        a = normed(h.astype(F32))
        a1[ts] = a
        at[:, ts] = a.T
        return 0

    lax.fori_loop(0, NT, middle, 0)

    def backward(layer, a_ref, k):
        j = layer * NK + k
        q = (1 - layer) * NK + k
        if layer == 1:
            from_partner(j).wait_recv()
        prepare(j, False, layer == 1)
        gd[...] = jnp.zeros_like(gd)
        ggu[...] = jnp.zeros_like(ggu)

        def step(t, _):
            if layer == 1:
                ag_hooks(j, t)
            rs_hooks(q, t)
            ts = tokens(t)
            gu = dot(a_ref[ts], wgu[...])
            by_hidden = dot(by[ts], wdt[...]).astype(BF16).astype(F32)
            gate, up = gu[:, :C], gu[:, C:]
            s = 1.0 / (1.0 + jnp.exp(-gate))
            silu = gate * s
            hidden = (silu * up).astype(BF16)
            by_up = (by_hidden * silu).astype(BF16)
            by_gate = (by_hidden * up * (s + silu * (1.0 - s))).astype(BF16)
            both = jnp.concatenate([by_gate, by_up], axis=1)
            gd[...] += dot(byt[:, ts], hidden)
            ggu[...] += dot(at[:, ts], both)
            if layer == 1:
                part = dot(both, wt[...])

                @pl.when(k == 0)
                def _():
                    acc[ts] = part

                @pl.when(k != 0)
                def _():
                    acc[ts] += part

            return 0

        lax.fori_loop(0, NT, step, 0)
        rs_begin(q)

    lax.fori_loop(0, NK, lambda k, _: (backward(1, a1, k), 0)[1], 0)

    def between(t, _):
        ts = tokens(t)
        wide = h1[ts].astype(F32)
        g = acc[ts].astype(BF16).astype(F32)
        s = lax.rsqrt(jnp.mean(wide * wide, -1, keepdims=True) + 1e-6)
        m = jnp.mean(g * wide, -1, keepdims=True)
        back = (g * s - wide * (s * s * s * m)).astype(BF16)
        total = (back.astype(F32) + by[ts].astype(F32)).astype(BF16)
        by[ts] = total
        byt[:, ts] = total.T
        at[:, ts] = a0[ts].T
        return 0

    lax.fori_loop(0, NT, between, 0)
    lax.fori_loop(0, NK, lambda k, _: (backward(0, a0, k), 0)[1], 0)

    last = jnp.int32(NJ - 1)
    rs_final(last - 1)
    rs_chip(last)
    rs_relay(last)
    rs_final(last)

    def squares(i):
        return pltpu.make_async_remote_copy(
            src_ref=sq, dst_ref=nb.at[i - 1], send_sem=n_send.at[i - 1], recv_sem=n_recv.at[i - 1],
            device_id=(rep, (dp + i) % DEV), device_id_type=MESH)

    for i in range(1, DEV):
        squares(i).start()
    total = sq[...]
    for i in range(1, DEV):
        squares(i).wait_recv()
        total += nb[i - 1]
    sq_out[...] = total
    for i in range(1, DEV):
        squares(i).wait_send()
    for q in (NJ - 2, NJ - 1):
        exchange(q).wait_send()
        wait_z_sends(q)

    def drain(j, _):
        for i in (1, 2, 3):
            along_z(j, i).wait_send()
            for q in (1, 2, 3):
                across(j, i, q).wait_send()
        to_partner(j).wait_send()
        return 0

    lax.fori_loop(0, NJ, drain, 0)


def gradients_of(x, dy, pack):
    vm = pltpu.VMEM
    dma = pltpu.SemaphoreType.DMA
    scratch = [
        vm((NJ, 2, 4, ROWS, C), BF16),
        vm((T, D), BF16),
        vm((T, D), BF16),
        vm((D, T), BF16),
        vm((T, D), BF16),
        vm((D, T), BF16),
        vm((T, D), BF16),
        vm((T, D), F32),
        vm((D, 2 * C), BF16),
        vm((C, D), BF16),
        vm((D, C), BF16),
        vm((2 * C, D), BF16),
        vm((D, C), F32),
        vm((D, 2 * C), F32),
        vm((2, 2, 4, ROWS, C), BF16),
        vm((NJ, 4, ROWS, C), BF16),
        vm((2, 4, ROWS, C), BF16),
        vm((NJ, ROWS, C), BF16),
        vm((NJ, 3, ROWS, C), BF16),
        vm((8, C), F32),
        vm((DEV - 1, 8, C), F32),
        dma((3,)),
        dma((NJ, 3)), dma((NJ, 3)),
        dma((NJ, 3, 3)), dma((NJ, 3, 3)),
        dma((NJ,)), dma((NJ,)),
        dma((NJ,)), dma((NJ,)),
        dma((NJ, 3)), dma((NJ, 3)),
        dma((NJ,)),
        dma((DEV - 1,)), dma((DEV - 1,)),
    ]
    any_space = pl.BlockSpec(memory_space=pl.ANY)
    vmem = pl.BlockSpec(memory_space=pltpu.VMEM)
    return pl.pallas_call(
        kernel,
        out_shape=(jax.ShapeDtypeStruct((NJ, ROWS, C), BF16), jax.ShapeDtypeStruct((8, C), F32)),
        in_specs=[any_space] * 3,
        out_specs=(vmem, vmem),
        scratch_shapes=scratch,
        compiler_params=pltpu.CompilerParams(collective_id=0, has_side_effects=True, vmem_limit_bytes=67_043_328),
    )(x, dy, pack)


def spread(w):
    w = w.reshape(2, 64, DEV, FF // DEV)
    w = jnp.pad(w, ((0, 0), (0, 0), (0, 0), (0, NK * SH - FF // DEV)))
    return w.reshape(2, 64, DEV, NK, SH).transpose(0, 3, 1, 2, 4).reshape(2, NK, 64, C)


def gathered_back(g):
    g = g.reshape(2, NK, 64, DEV, SH).transpose(0, 2, 3, 1, 4).reshape(2, 64, DEV, NK * SH)
    return g[..., : FF // DEV].reshape(2, 64, FF)


def packed(wg, wu, wd):
    down = jnp.pad(wd, ((0, 0), (0, NK * SH - FF // DEV), (0, 0))).reshape(2, NK, SH, 2, C)
    down = down.transpose(0, 1, 3, 2, 4).reshape(2, NK, 2 * SH, C)
    return jnp.concatenate([spread(wg), spread(wu), down], 2).reshape(NJ, ROWS, C)


def unpacked(g):
    g = g.reshape(2, NK, ROWS, C)[::-1]
    down = g[:, :, 128:].reshape(2, NK, 2, SH, C).transpose(0, 1, 3, 2, 4).reshape(2, NK * SH, D)
    return gathered_back(g[:, :, :64]), gathered_back(g[:, :, 64:128]), down[:, : FF // DEV]


def adamw(w, m, v, g):
    m = 0.9 * m + 0.1 * g
    v = 0.95 * v + 0.05 * g * g
    step = m * lax.rsqrt(v + 1e-8) + 0.1 * w
    return (w - 0.02 * step).astype(BF16), m, v


def solution(mesh):
    def step(x, dy, *arrays):
        weights, m, v = (arrays[i : i + 3] for i in (0, 3, 6))
        g, squares = gradients_of(x[0], dy[0], packed(*weights))
        count = 3 * 2 * D * FF
        factor = jnp.minimum(1.0, 0.5 * lax.rsqrt(jnp.sum(squares) / count + 1e-30))
        new = [
            adamw(w.astype(F32), m, v, g.astype(F32) * factor)
            for w, m, v, g in zip(weights, m, v, unpacked(g), strict=True)
        ]
        return tuple(one[which] for which in range(3) for one in new)

    states, cut = P(("rep", "dp"), None, None), P(None, "dp", None)
    return jax.shard_map(
        step,
        mesh=mesh,
        in_specs=(states, states) + (cut,) * 9,
        out_specs=(P("rep", "dp", None),) * 9,
        check_vma=False,
    )
```

```python
import functools

import jax
import jax.numpy as jnp
from jax import lax
from jax.experimental import pallas as pl
from jax.experimental.pallas import tpu as pltpu
from jax.sharding import PartitionSpec as P

MESH = pl.DeviceIdType.MESH
F32, BF16 = jnp.float32, jnp.bfloat16
T, D, FF = 4096, 512, 1408
DEV = 8
C = 256
NK = 6
NJ = 2 * NK
SH = C // DEV
SHARE = FF // DEV
ROWS = 192
GATE, UP, LOW, HIGH = slice(0, 64), slice(64, 128), slice(128, 160), slice(160, 192)
LEFT, RIGHT = slice(0, C), slice(C, 2 * C)
TB = 512
NT = T // TB
NT_DIMS = (((1,), (1,)), ((), ()))
RB = 32


def normed(wide):
    scale = lax.rsqrt(jnp.mean(wide * wide, -1, keepdims=True) + 1e-6)
    return (wide * scale).astype(BF16)


def placement(k):
    place, unit = (lax.broadcasted_iota(jnp.int32, (C, FF), axis) for axis in range(2))
    own = k * SH + lax.rem(place, SH)
    return jnp.where((unit == lax.div(place, SH) * SHARE + own) & (own < SHARE), 1.0, 0.0).astype(BF16)


def dot(a, b):
    return jnp.dot(a, b, preferred_element_type=F32)


def kernel(
    x_hbm, dy_hbm, wg, wu, wdown, g_out, sq_out, kept,
    wbuf, a0, a1, at, by, byt, h1, acc, wgu, wd, wdt, wt, gd, ggu, gu, dh, hid, both, pg, rx, tx, rl, rz, sq, nb,
    local_sem, k_sem, s1_send, s1_recv, s2_send, s2_recv, s3_send, s3_recv,
    d_send, d_recv, z_send, z_recv, r_recv, n_send, n_recv,
):
    rep, dp = lax.axis_index("rep"), lax.axis_index("dp")
    z, c = dp // 2, dp % 2
    partner = z * 2 + (1 - c)
    outer = (z == 0) | (z == 3)
    inner = (z == 1) | (z == 2)
    near, far, opposite = 1 + z // 3, 2 - z // 3, 3 - z
    other_outer = 3 * (z - 1)
    other_outer = jnp.where(inner, other_outer, 0)
    far_outer = 3 - other_outer

    copies = [
        pltpu.make_async_copy(x_hbm, h1, local_sem.at[0]),
        pltpu.make_async_copy(dy_hbm, by, local_sem.at[1]),
    ]
    for copy in copies:
        copy.start()
    barrier = pltpu.get_barrier_semaphore()
    for i in range(1, DEV):
        pl.semaphore_signal(barrier, inc=1, device_id=(rep, (dp + i) % DEV), device_id_type=MESH)
    for i in range(1, 4):
        pl.semaphore_signal(barrier, inc=1, device_id=((rep + i) % 4, dp), device_id_type=MESH)

    def quarter(j, zz, rr):
        return wbuf.at[j, c, zz, pl.ds(pl.multiple_of(rr * (ROWS // 4), 16), ROWS // 4)]

    def along_z(j, i):
        ref = quarter(j, z, rep)
        return pltpu.make_async_remote_copy(
            src_ref=ref, dst_ref=ref, send_sem=s1_send.at[j, i - 1], recv_sem=s1_recv.at[j, i - 1],
            device_id=(rep, ((z + i) % 4) * 2 + c), device_id_type=MESH)

    def from_z(j, i):
        ref = quarter(j, (z + 4 - i) % 4, rep)
        return pltpu.make_async_remote_copy(
            src_ref=ref, dst_ref=ref, send_sem=s1_send.at[j, i - 1], recv_sem=s1_recv.at[j, i - 1],
            device_id=(rep, dp), device_id_type=MESH)

    def across(j, i, q):
        ref = quarter(j, (z + 4 - i) % 4, rep)
        return pltpu.make_async_remote_copy(
            src_ref=ref, dst_ref=ref, send_sem=s2_send.at[j, i - 1, q - 1], recv_sem=s2_recv.at[j, i - 1, q - 1],
            device_id=((rep + q) % 4, dp), device_id_type=MESH)

    def from_across(j, i, q):
        ref = quarter(j, (z + 4 - i) % 4, (rep + 4 - q) % 4)
        return pltpu.make_async_remote_copy(
            src_ref=ref, dst_ref=ref, send_sem=s2_send.at[j, i - 1, q - 1], recv_sem=s2_recv.at[j, i - 1, q - 1],
            device_id=(rep, dp), device_id_type=MESH)

    def to_partner(j):
        ref = wbuf.at[j, c]
        return pltpu.make_async_remote_copy(
            src_ref=ref, dst_ref=ref, send_sem=s3_send.at[j], recv_sem=s3_recv.at[j],
            device_id=(rep, partner), device_id_type=MESH)

    def from_partner(j):
        ref = wbuf.at[j, 1 - c]
        return pltpu.make_async_remote_copy(
            src_ref=ref, dst_ref=ref, send_sem=s3_send.at[j], recv_sem=s3_recv.at[j],
            device_id=(rep, dp), device_id_type=MESH)

    def stage_one(j):
        for i in (1, 2, 3):
            along_z(j, i).start()

    def stage_two(j):
        for i in (1, 2, 3):
            from_z(j, i).wait_recv()
            for q in (1, 2, 3):
                across(j, i, q).start()

    def stage_three(j):
        for i in (1, 2, 3):
            for q in (1, 2, 3):
                from_across(j, i, q).wait_recv()
        to_partner(j).start()

    def pack(k):
        places = placement(k)
        for part, w in ((GATE, wg), (UP, wu)):
            moved = lax.dot_general(w[...].reshape(-1, FF), places, NT_DIMS, preferred_element_type=F32).astype(BF16)
            for layer in range(2):
                wbuf[layer * NK + k, c, z, part] = moved[layer * 64 : layer * 64 + 64]
        have = min(SH, SHARE - k * SH)
        for layer in range(2):
            rows = wdown[layer, k * SH : k * SH + have]
            if have < SH:
                rows = jnp.concatenate([rows, jnp.zeros((SH - have, D), BF16)])
            wbuf[layer * NK + k, c, z, LOW] = rows[:, LEFT]
            wbuf[layer * NK + k, c, z, HIGH] = rows[:, RIGHT]

    pack(0)
    pl.semaphore_wait(barrier, DEV - 1 + 3)
    for k in range(1, NK):
        pack(k)
        stage_one(k - 1)
    lax.fori_loop(NK - 1, NJ, lambda j, _: (stage_one(j), 0)[1], 0)

    def exchange(q):
        return pltpu.make_async_remote_copy(
            src_ref=pg.at[q % 2, 1 - c], dst_ref=rx.at[q % 4], send_sem=d_send.at[q], recv_sem=d_recv.at[q],
            device_id=(rep, partner), device_id_type=MESH)

    def z_copy(q, block, dst, recv_sem, n, zz):
        return pltpu.make_async_remote_copy(
            src_ref=tx.at[q % 2, block], dst_ref=dst, send_sem=z_send.at[q, n], recv_sem=recv_sem,
            device_id=(rep, zz * 2 + c), device_id_type=MESH)

    def chip_sum(q, block):
        return pg[q % 2, c, block].astype(F32) + rx[q % 4, block].astype(F32)

    def wait_z_sends(q):
        for n in range(3):
            z_copy(q, 0, rz.at[q % 4, 0], z_recv.at[q, 0], n, z).wait_send()

    def rs_chip(q):
        exchange(q).wait_recv()

        @pl.when(q >= 2)
        def _():
            wait_z_sends(q - 2)

        for block in range(4):
            tx[q % 2, block] = chip_sum(q, block).astype(BF16)

        @pl.when(outer)
        def _():
            z_copy(q, opposite, rl.at[q % 4], r_recv.at[q], 0, near).start()
            z_copy(q, far, rz.at[q % 4, 1], z_recv.at[q, 1], 1, far).start()
            z_copy(q, near, rz.at[q % 4, 0], z_recv.at[q, 0], 2, near).start()

        @pl.when(inner)
        def _():
            z_copy(q, opposite, rz.at[q % 4, 2], z_recv.at[q, 2], 0, opposite).start()
            z_copy(q, other_outer, rz.at[q % 4, 0], z_recv.at[q, 0], 1, other_outer).start()

    def rs_relay(q):
        @pl.when(inner)
        def _():
            z_copy(q, 0, rl.at[q % 4], r_recv.at[q], 2, z).wait_recv()
            tx[q % 2, far_outer] = (chip_sum(q, far_outer) + rl[q % 4].astype(F32)).astype(BF16)
            z_copy(q, far_outer, rz.at[q % 4, 1], z_recv.at[q, 1], 2, far_outer).start()

    def rs_final(q):
        for n in range(2):
            z_copy(q, 0, rz.at[q % 4, n], z_recv.at[q, n], 0, z).wait_recv()
        total = chip_sum(q, z) + rz[q % 4, 0].astype(F32) + rz[q % 4, 1].astype(F32)

        def finish(value):
            rounded = value.astype(BF16)
            g_out[q] = rounded
            wide = rounded.astype(F32)
            sq[...] += jnp.sum((wide * wide).reshape(ROWS // 8, 8, C), 0)

        @pl.when(outer)
        def _():
            finish(total)

        @pl.when(inner)
        def _():
            z_copy(q, 0, rz.at[q % 4, 2], z_recv.at[q, 2], 0, z).wait_recv()
            finish(total + rz[q % 4, 2].astype(F32))

    def rs_begin(q):
        @pl.when(q >= 2)
        def _():
            exchange(q - 2).wait_send()

        for d in range(DEV):
            rows = slice(d * 64, d * 64 + 64)
            pg[q % 2, d % 2, d // 2, GATE] = ggu[rows, LEFT].astype(BF16)
            pg[q % 2, d % 2, d // 2, UP] = ggu[rows, RIGHT].astype(BF16)
        turned = gd[...].astype(BF16).T
        for d in range(DEV):
            rows = slice(d * SH, d * SH + SH)
            pg[q % 2, d % 2, d // 2, LOW] = turned[rows, LEFT]
            pg[q % 2, d % 2, d // 2, HIGH] = turned[rows, RIGHT]
        exchange(q).start()

    def load_gate_up(j):
        for d in range(DEV):
            rows = slice(d * 64, d * 64 + 64)
            wgu[rows, LEFT] = wbuf[j, d % 2, d // 2, GATE]
            wgu[rows, RIGHT] = wbuf[j, d % 2, d // 2, UP]

    def load_down(j):
        for d in range(DEV):
            rows = slice(d * SH, d * SH + SH)
            wd[rows, LEFT] = wbuf[j, d % 2, d // 2, LOW]
            wd[rows, RIGHT] = wbuf[j, d % 2, d // 2, HIGH]

    def tokens(t):
        return pl.ds(pl.multiple_of(t * TB, TB), TB)

    def ag_two(j):
        @pl.when(j + 3 < NJ)
        def _():
            stage_two(j + 3)

    def ag_three(j):
        @pl.when(j + 1 < NJ)
        def _():
            stage_three(j + 1)

    sq[...] = jnp.zeros_like(sq)
    for copy in copies:
        copy.wait()

    def first(t, _):
        ts = tokens(t)
        a0[ts] = normed(h1[ts].astype(F32))
        byt[:, ts] = by[ts].T
        acc[ts] = jnp.zeros((TB, D), F32)

        @pl.when(t >= NT - 3)
        def _():
            stage_two(t - (NT - 3))

        return 0

    lax.fori_loop(0, NT, first, 0)
    stage_three(0)

    def together(*lists):
        order = sorted((n / len(one), m, n) for m, one in enumerate(lists) for n in range(len(one)))
        for _, m, n in order:
            lists[m][n]()

    def gate_up(a_ref, t, slot):
        def product(n):
            cols = slice(n * C, n * C + C)
            gu[slot, :, cols] = dot(a_ref[tokens(t)], wgu[:, cols])

        return [functools.partial(product, n) for n in range(2)]

    def of_hidden(t, slot):
        def product():
            dh[slot] = dot(by[tokens(t)], wdt[...]).astype(BF16)

        return [product]

    def elementwise(gu_slot, slot, hidden_gradient):
        def piece(n):
            rows = slice(n * RB, n * RB + RB)
            gate, up = gu[gu_slot, rows, LEFT], gu[gu_slot, rows, RIGHT]
            s = 1.0 / (1.0 + jnp.exp(-gate))
            silu = gate * s
            hid[slot, rows] = (silu * up).astype(BF16)
            if hidden_gradient:
                by_hidden = dh[slot, rows].astype(F32)
                both[slot, rows, RIGHT] = (by_hidden * silu).astype(BF16)
                both[slot, rows, LEFT] = (by_hidden * up * (s + silu * (1.0 - s))).astype(BF16)

        return [functools.partial(piece, n) for n in range(TB // RB)]

    def forward_products(t, slot):
        ts = tokens(t)

        def down(n):
            cols = slice(n * C, n * C + C)
            acc[ts, cols] += dot(hid[slot], wd[:, cols])

        return [functools.partial(down, n) for n in range(2)]

    def last_products(t, slot, input_gradient):
        ts = tokens(t)

        def of_down():
            gd[...] += dot(byt[:, ts], hid[slot])

        def of_gate_up(n):
            cols = slice(n * C, n * C + C)
            ggu[:, cols] += dot(at[:, ts], both[slot, :, cols])

        def of_input(n):
            cols = slice(n * C, n * C + C)
            acc[ts, cols] += dot(both[slot], wt[:, cols])

        parts = [of_down] + [functools.partial(of_gate_up, n) for n in range(2)]
        return parts + [functools.partial(of_input, n) for n in range(2)] if input_gradient else parts

    def run(j0, for_one, for_three, one, two, three, hook, finish):
        for_one(j0)
        together(one(j0, 0))
        together(one(j0, 1), two(j0, 0))
        for_three(j0)

        def chunk(k, _):
            j = j0 + k
            following = j0 + jnp.minimum(k + 1, NK - 1)
            for t in range(1, NT - 1):
                if t % 2:
                    hook(k, t // 2)
                together(one(j, t + 1), two(j, t), three(t - 1))
            hook(k, NT // 2 - 1)
            for_one(following)
            together(one(following, 0), two(j, NT - 1), three(NT - 2))
            together(one(following, 1), two(following, 0), three(NT - 1))
            finish(k)
            for_three(following)
            return 0

        lax.fori_loop(0, NK, chunk, 0)

    def keep(k, t):
        return pltpu.make_async_copy(gu.at[t % 4], kept.at[k, t], k_sem.at[t % 4])

    def fetch(k, t):
        return pltpu.make_async_copy(kept.at[k, t], gu.at[t % 4], k_sem.at[t % 4])

    def arrive(j):
        from_partner(j).wait_recv()

    def forward_hook(k, n):
        if n == 0:
            ag_two(k)
        if n == 1:
            ag_three(k)
        if n == 3:
            arrive(k + 1)

    def forward_one(k, t):
        def free():
            keep(k, t).wait()

        parts = gate_up(a0, t, t % 4)
        return parts if isinstance(k, int) else [free] + parts

    def forward_two(k, t):
        parts = elementwise(t % 4, t % 2, False)
        return parts[:4] + [keep(k, t).start] + parts[4:]

    arrive(0)
    for t in (2, 3):
        gu[t] = jnp.zeros((TB, 2 * C), F32)
        keep(0, t).start()
    run(
        0, load_gate_up, load_down,
        forward_one, forward_two,
        lambda t: forward_products(t, t % 2),
        forward_hook,
        lambda k: None,
    )
    for t in (0, 2, 3):
        keep(0, t).wait()

    def middle(t, _):
        ts = tokens(t)
        h = (h1[ts].astype(F32) + acc[ts].astype(BF16).astype(F32)).astype(BF16)
        acc[ts] = jnp.zeros((TB, D), F32)
        h1[ts] = h
        a = normed(h.astype(F32))
        a1[ts] = a
        at[:, ts] = a.T
        return 0

    lax.fori_loop(0, NT, middle, 0)

    def backward(layer):
        j0, q0 = layer * NK, (1 - layer) * NK

        def for_one(j):
            if layer == 1:
                load_gate_up(j)
            load_down(j)
            wdt[...] = wd[...].T

        def for_three(j):
            if layer == 1:
                wt[...] = wgu[...].T

        def hook(k, n):
            j, q = j0 + k, q0 + k
            if layer == 1 and n == 0:
                ag_two(j)
            if layer == 1 and n == 1:
                ag_three(j)
            if layer == 1 and n == 3:
                @pl.when(k + 1 < NK)
                def _():
                    arrive(j + 1)

            @pl.when(q >= 1)
            def _():
                if n == 1:
                    rs_chip(q - 1)
                if n == 3:
                    rs_relay(q - 1)

            @pl.when(q >= 2)
            def _():
                if n == 2:
                    rs_final(q - 2)

        def clear():
            gd[...] = jnp.zeros_like(gd)
            ggu[...] = jnp.zeros_like(ggu)

        def finish(k):
            rs_begin(q0 + k)
            clear()

        clear()
        if layer == 1:
            run(
                j0, for_one, for_three,
                lambda j, t: gate_up(a1, t, t % 4) + of_hidden(t, t % 2),
                lambda j, t: elementwise(t % 4, t % 2, True),
                lambda t: last_products(t, t % 2, True),
                hook,
                finish,
            )
        else:
            def two(k, t):
                ahead = t + 3
                after = k if ahead < NT else jnp.minimum(k + 1, NK - 1)
                parts = elementwise(t % 4, t % 2, True)
                return [fetch(after, ahead % NT).start, fetch(k, t).wait] + parts

            run(
                0, for_one, for_three,
                lambda k, t: of_hidden(t, t % 2),
                two,
                lambda t: last_products(t, t % 2, False),
                hook,
                finish,
            )
            for t in (1, 2, 3):
                fetch(0, t).wait()

    backward(1)

    def between(t, _):
        ts = tokens(t)
        wide = h1[ts].astype(F32)
        g = acc[ts].astype(BF16).astype(F32)
        s = lax.rsqrt(jnp.mean(wide * wide, -1, keepdims=True) + 1e-6)
        m = jnp.mean(g * wide, -1, keepdims=True)
        back = (g * s - wide * (s * s * s * m)).astype(BF16)
        total = (back.astype(F32) + by[ts].astype(F32)).astype(BF16)
        by[ts] = total
        byt[:, ts] = total.T
        at[:, ts] = a0[ts].T
        return 0

    for t in range(3):
        fetch(0, t).start()
    lax.fori_loop(0, NT, between, 0)
    backward(0)

    last = jnp.int32(NJ - 1)
    rs_final(last - 1)
    rs_chip(last)
    rs_relay(last)
    rs_final(last)

    def squares(i):
        return pltpu.make_async_remote_copy(
            src_ref=sq, dst_ref=nb.at[i - 1], send_sem=n_send.at[i - 1], recv_sem=n_recv.at[i - 1],
            device_id=(rep, (dp + i) % DEV), device_id_type=MESH)

    for i in range(1, DEV):
        squares(i).start()
    total = sq[...]
    for i in range(1, DEV):
        squares(i).wait_recv()
        total += nb[i - 1]
    sq_out[...] = total
    for i in range(1, DEV):
        squares(i).wait_send()
    for q in (NJ - 2, NJ - 1):
        exchange(q).wait_send()
        wait_z_sends(q)

    def drain(j, _):
        for i in (1, 2, 3):
            along_z(j, i).wait_send()
            for q in (1, 2, 3):
                across(j, i, q).wait_send()
        to_partner(j).wait_send()
        return 0

    lax.fori_loop(0, NJ, drain, 0)


def gradients_of(x, dy, *weights):
    vm = pltpu.VMEM
    dma = pltpu.SemaphoreType.DMA
    scratch = [
        vm((NJ, 2, 4, ROWS, C), BF16),
        vm((T, D), BF16),
        vm((T, D), BF16),
        vm((D, T), BF16),
        vm((T, D), BF16),
        vm((D, T), BF16),
        vm((T, D), BF16),
        vm((T, D), F32),
        vm((D, 2 * C), BF16),
        vm((C, D), BF16),
        vm((D, C), BF16),
        vm((2 * C, D), BF16),
        vm((D, C), F32),
        vm((D, 2 * C), F32),
        vm((4, TB, 2 * C), F32),
        vm((2, TB, C), BF16),
        vm((2, TB, C), BF16),
        vm((2, TB, 2 * C), BF16),
        vm((2, 2, 4, ROWS, C), BF16),
        vm((4, 4, ROWS, C), BF16),
        vm((2, 4, ROWS, C), BF16),
        vm((4, ROWS, C), BF16),
        vm((4, 3, ROWS, C), BF16),
        vm((8, C), F32),
        vm((DEV - 1, 8, C), F32),
        dma((2,)), dma((4,)),
        dma((NJ, 3)), dma((NJ, 3)),
        dma((NJ, 3, 3)), dma((NJ, 3, 3)),
        dma((NJ,)), dma((NJ,)),
        dma((NJ,)), dma((NJ,)),
        dma((NJ, 3)), dma((NJ, 3)),
        dma((NJ,)),
        dma((DEV - 1,)), dma((DEV - 1,)),
    ]
    any_space = pl.BlockSpec(memory_space=pl.ANY)
    vmem = pl.BlockSpec(memory_space=pltpu.VMEM)
    return pl.pallas_call(
        kernel,
        out_shape=(jax.ShapeDtypeStruct((NJ, ROWS, C), BF16), jax.ShapeDtypeStruct((8, C), F32),
                   jax.ShapeDtypeStruct((NK, NT, TB, 2 * C), F32)),
        in_specs=[any_space] * 2 + [vmem] * 3,
        out_specs=(vmem, vmem, any_space),
        scratch_shapes=scratch,
        compiler_params=pltpu.CompilerParams(collective_id=0, has_side_effects=True, vmem_limit_bytes=67_043_328),
    )(x, dy, *weights)


def adamw(w, m, v, g):
    m = 0.9 * m + 0.1 * g
    v = 0.95 * v + 0.05 * g * g
    step = m * lax.rsqrt(v + 1e-8) + 0.1 * w
    return (w - 0.02 * step).astype(BF16), m, v


def update(g, squares, *refs):
    ins, outs, held, (places, came, in_sem, out_sem) = refs[:9], refs[9:18], refs[18:27], refs[27:]
    copies = [pltpu.make_async_copy(a, b, in_sem.at[n]) for n, (a, b) in enumerate(zip(ins, held))]
    puts = [pltpu.make_async_copy(b, a, out_sem.at[n]) for n, (a, b) in enumerate(zip(outs, held))]
    for copy in copies:
        copy.start()
    for k in range(NK):
        places[k * C : k * C + C] = placement(k)
    count = 3 * 2 * D * FF
    factor = jnp.minimum(1.0, 0.5 * lax.rsqrt(jnp.sum(squares[...], keepdims=True) / count + 1e-30))
    chunks = [
        jnp.concatenate([g[NK + k, GATE], g[NK + k, UP], g[k, GATE], g[k, UP]]) for k in range(NK)
    ]
    came[...] = dot(jnp.concatenate(chunks, 1), places[...])
    for n in range(3):
        for which in range(n, 9, 3):
            copies[which].wait()
        w, m, v = held[n::3]
        step = SH // 2
        for layer in range(2):
            for row in range(0, w.shape[1], step):
                rows = slice(row, row + step)
                if n < 2:
                    first = (layer * 2 + n) * 64 + row
                    part = came[first : first + step]
                else:
                    q, inside = (1 - layer) * NK + row // SH, row % SH
                    part = jnp.concatenate(
                        [g[q, one.start + inside : one.start + inside + step] for one in (LOW, HIGH)], 1
                    ).astype(F32)
                w[layer, rows], m[layer, rows], v[layer, rows] = adamw(
                    w[layer, rows].astype(F32), m[layer, rows], v[layer, rows], part * factor
                )
        for which in range(n, 9, 3):
            puts[which].start()
    for put in puts:
        put.wait()


def updated(g, squares, arrays):
    any_space, vmem = pl.BlockSpec(memory_space=pl.ANY), pl.BlockSpec(memory_space=pltpu.VMEM)
    like = [jax.ShapeDtypeStruct(a.shape, a.dtype) for a in arrays]
    return pl.pallas_call(
        update,
        out_shape=like,
        in_specs=[vmem] * 2 + [any_space] * 9,
        out_specs=[any_space] * 9,
        scratch_shapes=[pltpu.VMEM(a.shape, a.dtype) for a in arrays]
        + [
            pltpu.VMEM((NK * C, FF), BF16),
            pltpu.VMEM((4 * 64, FF), F32),
            pltpu.SemaphoreType.DMA((9,)),
            pltpu.SemaphoreType.DMA((9,)),
        ],
        compiler_params=pltpu.CompilerParams(vmem_limit_bytes=60_000_000),
    )(g, squares, *arrays)


def solution(mesh):
    def step(x, dy, *arrays):
        g, squares, _ = gradients_of(x[0], dy[0], *arrays[:3])
        return tuple(updated(g, squares, arrays))

    states, cut = P(("rep", "dp"), None, None), P(None, "dp", None)
    return jax.shard_map(
        step,
        mesh=mesh,
        in_specs=(states, states) + (cut,) * 9,
        out_specs=(P("rep", "dp", None),) * 9,
        check_vma=False,
    )
```

```python
import functools

import jax
import jax.numpy as jnp
from jax import lax
from jax.experimental import pallas as pl
from jax.experimental.pallas import tpu as pltpu
from jax.sharding import PartitionSpec as P

MESH = pl.DeviceIdType.MESH
F32, BF16 = jnp.float32, jnp.bfloat16
T, D, FF = 4096, 512, 1408
DEV = 8
C = 256
NK = 6
NJ = 2 * NK
SH = C // DEV
SHARE = FF // DEV
ROWS = 192
GATE, UP, LOW, HIGH = slice(0, 64), slice(64, 128), slice(128, 160), slice(160, 192)
LEFT, RIGHT = slice(0, C), slice(C, 2 * C)
TB = 512
NT = T // TB
NT_DIMS = (((1,), (1,)), ((), ()))
RB = 32


def normed(wide):
    scale = lax.rsqrt(jnp.mean(wide * wide, -1, keepdims=True) + 1e-6)
    return (wide * scale).astype(BF16)


def placement(k):
    place, unit = (lax.broadcasted_iota(jnp.int32, (C, FF), axis) for axis in range(2))
    own = k * SH + lax.rem(place, SH)
    return jnp.where((unit == lax.div(place, SH) * SHARE + own) & (own < SHARE), 1.0, 0.0).astype(BF16)


def dot(a, b):
    return jnp.dot(a, b, preferred_element_type=F32)


def kernel(
    x_hbm, dy_hbm, wg, wu, wdown, g_out, sq_out, kept,
    wbuf, a0, a1, at, by, byt, h1, acc, wgu, wd, wdt, wt, gd, ggu, gu, dh, hid, both, pg, rx, tx, rl, rz, sq, nb,
    local_sem, k_sem, s1_send, s1_recv, s2_send, s2_recv, s3_send, s3_recv,
    d_send, d_recv, z_send, z_recv, r_recv, n_send, n_recv,
):
    rep, dp = lax.axis_index("rep"), lax.axis_index("dp")
    z, c = dp // 2, dp % 2
    partner = z * 2 + (1 - c)
    outer = (z == 0) | (z == 3)
    inner = (z == 1) | (z == 2)
    near, far, opposite = 1 + z // 3, 2 - z // 3, 3 - z
    other_outer = 3 * (z - 1)
    other_outer = jnp.where(inner, other_outer, 0)
    far_outer = 3 - other_outer

    copies = [
        pltpu.make_async_copy(x_hbm, h1, local_sem.at[0]),
        pltpu.make_async_copy(dy_hbm, by, local_sem.at[1]),
    ]
    for copy in copies:
        copy.start()
    barrier = pltpu.get_barrier_semaphore()
    for i in range(1, DEV):
        pl.semaphore_signal(barrier, inc=1, device_id=(rep, (dp + i) % DEV), device_id_type=MESH)
    for i in range(1, 4):
        pl.semaphore_signal(barrier, inc=1, device_id=((rep + i) % 4, dp), device_id_type=MESH)

    def quarter(j, zz, rr):
        return wbuf.at[j, c, zz, pl.ds(pl.multiple_of(rr * (ROWS // 4), 16), ROWS // 4)]

    def along_z(j, i):
        ref = quarter(j, z, rep)
        return pltpu.make_async_remote_copy(
            src_ref=ref, dst_ref=ref, send_sem=s1_send.at[j, i - 1], recv_sem=s1_recv.at[j, i - 1],
            device_id=(rep, ((z + i) % 4) * 2 + c), device_id_type=MESH)

    def from_z(j, i):
        ref = quarter(j, (z + 4 - i) % 4, rep)
        return pltpu.make_async_remote_copy(
            src_ref=ref, dst_ref=ref, send_sem=s1_send.at[j, i - 1], recv_sem=s1_recv.at[j, i - 1],
            device_id=(rep, dp), device_id_type=MESH)

    def across(j, i, q):
        ref = quarter(j, (z + 4 - i) % 4, rep)
        return pltpu.make_async_remote_copy(
            src_ref=ref, dst_ref=ref, send_sem=s2_send.at[j, i - 1, q - 1], recv_sem=s2_recv.at[j, i - 1, q - 1],
            device_id=((rep + q) % 4, dp), device_id_type=MESH)

    def from_across(j, i, q):
        ref = quarter(j, (z + 4 - i) % 4, (rep + 4 - q) % 4)
        return pltpu.make_async_remote_copy(
            src_ref=ref, dst_ref=ref, send_sem=s2_send.at[j, i - 1, q - 1], recv_sem=s2_recv.at[j, i - 1, q - 1],
            device_id=(rep, dp), device_id_type=MESH)

    def to_partner(j):
        ref = wbuf.at[j, c]
        return pltpu.make_async_remote_copy(
            src_ref=ref, dst_ref=ref, send_sem=s3_send.at[j], recv_sem=s3_recv.at[j],
            device_id=(rep, partner), device_id_type=MESH)

    def from_partner(j):
        ref = wbuf.at[j, 1 - c]
        return pltpu.make_async_remote_copy(
            src_ref=ref, dst_ref=ref, send_sem=s3_send.at[j], recv_sem=s3_recv.at[j],
            device_id=(rep, dp), device_id_type=MESH)

    def stage_one(j):
        for i in (1, 2, 3):
            along_z(j, i).start()

    def stage_two(j):
        for i in (1, 2, 3):
            from_z(j, i).wait_recv()
            for q in (1, 2, 3):
                across(j, i, q).start()

    def stage_three(j):
        for i in (1, 2, 3):
            for q in (1, 2, 3):
                from_across(j, i, q).wait_recv()
        to_partner(j).start()

    def pack(k):
        places = placement(k)
        for part, w in ((GATE, wg), (UP, wu)):
            moved = lax.dot_general(w[...].reshape(-1, FF), places, NT_DIMS, preferred_element_type=F32).astype(BF16)
            for layer in range(2):
                wbuf[layer * NK + k, c, z, part] = moved[layer * 64 : layer * 64 + 64]
        have = min(SH, SHARE - k * SH)
        for layer in range(2):
            rows = wdown[layer, k * SH : k * SH + have]
            if have < SH:
                rows = jnp.concatenate([rows, jnp.zeros((SH - have, D), BF16)])
            wbuf[layer * NK + k, c, z, LOW] = rows[:, LEFT]
            wbuf[layer * NK + k, c, z, HIGH] = rows[:, RIGHT]

    pack(0)
    pl.semaphore_wait(barrier, DEV - 1 + 3)
    for k in range(1, NK):
        pack(k)
        stage_one(k - 1)
    lax.fori_loop(NK - 1, NJ, lambda j, _: (stage_one(j), 0)[1], 0)

    def exchange(q):
        return pltpu.make_async_remote_copy(
            src_ref=pg.at[q % 3, 1 - c], dst_ref=rx.at[q % 4], send_sem=d_send.at[q], recv_sem=d_recv.at[q],
            device_id=(rep, partner), device_id_type=MESH)

    def z_copy(q, block, dst, recv_sem, n, zz):
        return pltpu.make_async_remote_copy(
            src_ref=tx.at[q % 3, block], dst_ref=dst, send_sem=z_send.at[q, n], recv_sem=recv_sem,
            device_id=(rep, zz * 2 + c), device_id_type=MESH)

    def chip_sum(q, block):
        return pg[q % 3, c, block].astype(F32) + rx[q % 4, block].astype(F32)

    def wait_z_sends(q):
        for n in range(3):
            z_copy(q, 0, rz.at[q % 4, 0], z_recv.at[q, 0], n, z).wait_send()

    def rs_chip(q):
        exchange(q).wait_recv()

        @pl.when(q >= 3)
        def _():
            wait_z_sends(q - 3)

        for block in range(4):
            tx[q % 3, block] = chip_sum(q, block).astype(BF16)

        @pl.when(outer)
        def _():
            z_copy(q, opposite, rl.at[q % 4], r_recv.at[q], 0, near).start()
            z_copy(q, far, rz.at[q % 4, 1], z_recv.at[q, 1], 1, far).start()
            z_copy(q, near, rz.at[q % 4, 0], z_recv.at[q, 0], 2, near).start()

        @pl.when(inner)
        def _():
            z_copy(q, opposite, rz.at[q % 4, 2], z_recv.at[q, 2], 0, opposite).start()
            z_copy(q, other_outer, rz.at[q % 4, 0], z_recv.at[q, 0], 1, other_outer).start()

    def rs_relay(q):
        @pl.when(inner)
        def _():
            z_copy(q, 0, rl.at[q % 4], r_recv.at[q], 2, z).wait_recv()
            tx[q % 3, far_outer] = (chip_sum(q, far_outer) + rl[q % 4].astype(F32)).astype(BF16)
            z_copy(q, far_outer, rz.at[q % 4, 1], z_recv.at[q, 1], 2, far_outer).start()

    def rs_final(q):
        for n in range(2):
            z_copy(q, 0, rz.at[q % 4, n], z_recv.at[q, n], 0, z).wait_recv()
        total = chip_sum(q, z) + rz[q % 4, 0].astype(F32) + rz[q % 4, 1].astype(F32)

        def finish(value):
            rounded = value.astype(BF16)
            g_out[q] = rounded
            wide = rounded.astype(F32)
            sq[...] += jnp.sum((wide * wide).reshape(ROWS // 8, 8, C), 0)

        @pl.when(outer)
        def _():
            finish(total)

        @pl.when(inner)
        def _():
            z_copy(q, 0, rz.at[q % 4, 2], z_recv.at[q, 2], 0, z).wait_recv()
            finish(total + rz[q % 4, 2].astype(F32))

    def rs_begin(q):
        @pl.when(q >= 3)
        def _():
            exchange(q - 3).wait_send()

        for d in range(DEV):
            rows = slice(d * 64, d * 64 + 64)
            pg[q % 3, d % 2, d // 2, GATE] = ggu[rows, LEFT].astype(BF16)
            pg[q % 3, d % 2, d // 2, UP] = ggu[rows, RIGHT].astype(BF16)
        turned = gd[...].astype(BF16).T
        for d in range(DEV):
            rows = slice(d * SH, d * SH + SH)
            pg[q % 3, d % 2, d // 2, LOW] = turned[rows, LEFT]
            pg[q % 3, d % 2, d // 2, HIGH] = turned[rows, RIGHT]
        exchange(q).start()

    def load_gate_up(j):
        for d in range(DEV):
            rows = slice(d * 64, d * 64 + 64)
            wgu[rows, LEFT] = wbuf[j, d % 2, d // 2, GATE]
            wgu[rows, RIGHT] = wbuf[j, d % 2, d // 2, UP]

    def load_down(j):
        for d in range(DEV):
            rows = slice(d * SH, d * SH + SH)
            wd[rows, LEFT] = wbuf[j, d % 2, d // 2, LOW]
            wd[rows, RIGHT] = wbuf[j, d % 2, d // 2, HIGH]

    def tokens(t):
        return pl.ds(pl.multiple_of(t * TB, TB), TB)

    def ag_two(j):
        @pl.when(j + 3 < NJ)
        def _():
            stage_two(j + 3)

    def ag_three(j):
        @pl.when(j + 1 < NJ)
        def _():
            stage_three(j + 1)

    sq[...] = jnp.zeros_like(sq)
    for copy in copies:
        copy.wait()

    def first(t, _):
        ts = tokens(t)
        a0[ts] = normed(h1[ts].astype(F32))
        byt[:, ts] = by[ts].T
        acc[ts] = jnp.zeros((TB, D), F32)

        @pl.when(t >= NT - 3)
        def _():
            stage_two(t - (NT - 3))

        return 0

    lax.fori_loop(0, NT, first, 0)
    stage_three(0)

    def together(*lists):
        order = sorted((n / len(one), m, n) for m, one in enumerate(lists) for n in range(len(one)))
        for _, m, n in order:
            lists[m][n]()

    def gate_up(a_ref, t, slot):
        def product(n):
            cols = slice(n * C, n * C + C)
            gu[slot, :, cols] = dot(a_ref[tokens(t)], wgu[:, cols])

        return [functools.partial(product, n) for n in range(2)]

    def of_hidden(t, slot):
        def product():
            dh[slot] = dot(by[tokens(t)], wdt[...]).astype(BF16)

        return [product]

    def elementwise(gu_slot, slot, hidden_gradient):
        def piece(n):
            rows = slice(n * RB, n * RB + RB)
            gate, up = gu[gu_slot, rows, LEFT], gu[gu_slot, rows, RIGHT]
            s = 1.0 / (1.0 + jnp.exp(-gate))
            silu = gate * s
            hid[slot, rows] = (silu * up).astype(BF16)
            if hidden_gradient:
                by_hidden = dh[slot, rows].astype(F32)
                both[slot, rows, RIGHT] = (by_hidden * silu).astype(BF16)
                both[slot, rows, LEFT] = (by_hidden * up * (s + silu * (1.0 - s))).astype(BF16)

        return [functools.partial(piece, n) for n in range(TB // RB)]

    def forward_products(t, slot):
        ts = tokens(t)

        def down(n):
            cols = slice(n * C, n * C + C)
            acc[ts, cols] += dot(hid[slot], wd[:, cols])

        return [functools.partial(down, n) for n in range(2)]

    def last_products(t, slot, input_gradient):
        ts = tokens(t)

        def of_down():
            gd[...] += dot(byt[:, ts], hid[slot])

        def of_gate_up(n):
            cols = slice(n * C, n * C + C)
            ggu[:, cols] += dot(at[:, ts], both[slot, :, cols])

        def of_input(n):
            cols = slice(n * C, n * C + C)
            acc[ts, cols] += dot(both[slot], wt[:, cols])

        parts = [of_down] + [functools.partial(of_gate_up, n) for n in range(2)]
        return parts + [functools.partial(of_input, n) for n in range(2)] if input_gradient else parts

    def run(j0, for_one, for_three, one, two, three, hook, finish):
        for_one(j0)
        together(one(j0, 0))
        together(one(j0, 1), two(j0, 0))
        for_three(j0)

        def chunk(k, _):
            j = j0 + k
            following = j0 + jnp.minimum(k + 1, NK - 1)
            for t in range(1, NT - 1):
                if t % 2:
                    hook(k, t // 2)
                together(one(j, t + 1), two(j, t), three(t - 1))
            hook(k, NT // 2 - 1)
            for_one(following)
            together(one(following, 0), two(j, NT - 1), three(NT - 2))
            together(one(following, 1), two(following, 0), three(NT - 1))
            finish(k)
            for_three(following)
            return 0

        lax.fori_loop(0, NK, chunk, 0)

    def keep(k, t):
        return pltpu.make_async_copy(gu.at[t % 4], kept.at[k, t], k_sem.at[t % 4])

    def fetch(k, t):
        return pltpu.make_async_copy(kept.at[k, t], gu.at[t % 4], k_sem.at[t % 4])

    def arrive(j):
        from_partner(j).wait_recv()

    def forward_hook(k, n):
        if n == 0:
            ag_two(k)
        if n == 1:
            ag_three(k)
        if n == 3:
            arrive(k + 1)

    def forward_one(k, t):
        def free():
            keep(k, t).wait()

        parts = gate_up(a0, t, t % 4)
        return parts if isinstance(k, int) else [free] + parts

    def forward_two(k, t):
        parts = elementwise(t % 4, t % 2, False)
        return parts[:4] + [keep(k, t).start] + parts[4:]

    arrive(0)
    for t in (2, 3):
        gu[t] = jnp.zeros((TB, 2 * C), F32)
        keep(0, t).start()
    run(
        0, load_gate_up, load_down,
        forward_one, forward_two,
        lambda t: forward_products(t, t % 2),
        forward_hook,
        lambda k: None,
    )
    for t in (0, 2, 3):
        keep(0, t).wait()

    def middle(t, _):
        ts = tokens(t)
        h = (h1[ts].astype(F32) + acc[ts].astype(BF16).astype(F32)).astype(BF16)
        acc[ts] = jnp.zeros((TB, D), F32)
        h1[ts] = h
        a = normed(h.astype(F32))
        a1[ts] = a
        at[:, ts] = a.T
        return 0

    lax.fori_loop(0, NT, middle, 0)

    def backward(layer):
        j0, q0 = layer * NK, (1 - layer) * NK

        def for_one(j):
            if layer == 1:
                load_gate_up(j)
            load_down(j)
            wdt[...] = wd[...].T

        def for_three(j):
            if layer == 1:
                wt[...] = wgu[...].T

        def hook(k, n):
            j, q = j0 + k, q0 + k
            if layer == 1 and n == 0:
                ag_two(j)
            if layer == 1 and n == 1:
                ag_three(j)
            if layer == 1 and n == 3:
                @pl.when(k + 1 < NK)
                def _():
                    arrive(j + 1)

            if n == 0:
                @pl.when(q >= 2)
                def _():
                    rs_relay(q - 2)

                @pl.when(q >= 3)
                def _():
                    rs_final(q - 3)

            if n == 1:
                @pl.when(q >= 1)
                def _():
                    rs_chip(q - 1)

        def clear():
            gd[...] = jnp.zeros_like(gd)
            ggu[...] = jnp.zeros_like(ggu)

        def finish(k):
            rs_begin(q0 + k)
            clear()

        clear()
        if layer == 1:
            run(
                j0, for_one, for_three,
                lambda j, t: gate_up(a1, t, t % 4) + of_hidden(t, t % 2),
                lambda j, t: elementwise(t % 4, t % 2, True),
                lambda t: last_products(t, t % 2, True),
                hook,
                finish,
            )
        else:
            def two(k, t):
                ahead = t + 3
                after = k if ahead < NT else jnp.minimum(k + 1, NK - 1)
                parts = elementwise(t % 4, t % 2, True)
                return [fetch(after, ahead % NT).start, fetch(k, t).wait] + parts

            run(
                0, for_one, for_three,
                lambda k, t: of_hidden(t, t % 2),
                two,
                lambda t: last_products(t, t % 2, False),
                hook,
                finish,
            )
            for t in (1, 2, 3):
                fetch(0, t).wait()

    backward(1)

    def between(t, _):
        ts = tokens(t)
        wide = h1[ts].astype(F32)
        g = acc[ts].astype(BF16).astype(F32)
        s = lax.rsqrt(jnp.mean(wide * wide, -1, keepdims=True) + 1e-6)
        m = jnp.mean(g * wide, -1, keepdims=True)
        back = (g * s - wide * (s * s * s * m)).astype(BF16)
        total = (back.astype(F32) + by[ts].astype(F32)).astype(BF16)
        by[ts] = total
        byt[:, ts] = total.T
        at[:, ts] = a0[ts].T
        return 0

    for t in range(3):
        fetch(0, t).start()
    lax.fori_loop(0, NT, between, 0)
    backward(0)

    last = jnp.int32(NJ - 1)
    rs_relay(last - 1)
    rs_final(last - 2)
    rs_chip(last)
    rs_final(last - 1)
    rs_relay(last)
    rs_final(last)

    def squares(i):
        return pltpu.make_async_remote_copy(
            src_ref=sq, dst_ref=nb.at[i - 1], send_sem=n_send.at[i - 1], recv_sem=n_recv.at[i - 1],
            device_id=(rep, (dp + i) % DEV), device_id_type=MESH)

    for i in range(1, DEV):
        squares(i).start()
    total = sq[...]
    for i in range(1, DEV):
        squares(i).wait_recv()
        total += nb[i - 1]
    sq_out[...] = total
    for i in range(1, DEV):
        squares(i).wait_send()
    for q in range(NJ - 3, NJ):
        exchange(q).wait_send()
        wait_z_sends(q)

    def drain(j, _):
        for i in (1, 2, 3):
            along_z(j, i).wait_send()
            for q in (1, 2, 3):
                across(j, i, q).wait_send()
        to_partner(j).wait_send()
        return 0

    lax.fori_loop(0, NJ, drain, 0)


def gradients_of(x, dy, *weights):
    vm = pltpu.VMEM
    dma = pltpu.SemaphoreType.DMA
    scratch = [
        vm((NJ, 2, 4, ROWS, C), BF16),
        vm((T, D), BF16),
        vm((T, D), BF16),
        vm((D, T), BF16),
        vm((T, D), BF16),
        vm((D, T), BF16),
        vm((T, D), BF16),
        vm((T, D), F32),
        vm((D, 2 * C), BF16),
        vm((C, D), BF16),
        vm((D, C), BF16),
        vm((2 * C, D), BF16),
        vm((D, C), F32),
        vm((D, 2 * C), F32),
        vm((4, TB, 2 * C), F32),
        vm((2, TB, C), BF16),
        vm((2, TB, C), BF16),
        vm((2, TB, 2 * C), BF16),
        vm((3, 2, 4, ROWS, C), BF16),
        vm((4, 4, ROWS, C), BF16),
        vm((3, 4, ROWS, C), BF16),
        vm((4, ROWS, C), BF16),
        vm((4, 3, ROWS, C), BF16),
        vm((8, C), F32),
        vm((DEV - 1, 8, C), F32),
        dma((2,)), dma((4,)),
        dma((NJ, 3)), dma((NJ, 3)),
        dma((NJ, 3, 3)), dma((NJ, 3, 3)),
        dma((NJ,)), dma((NJ,)),
        dma((NJ,)), dma((NJ,)),
        dma((NJ, 3)), dma((NJ, 3)),
        dma((NJ,)),
        dma((DEV - 1,)), dma((DEV - 1,)),
    ]
    any_space = pl.BlockSpec(memory_space=pl.ANY)
    vmem = pl.BlockSpec(memory_space=pltpu.VMEM)
    return pl.pallas_call(
        kernel,
        out_shape=(jax.ShapeDtypeStruct((NJ, ROWS, C), BF16), jax.ShapeDtypeStruct((8, C), F32),
                   jax.ShapeDtypeStruct((NK, NT, TB, 2 * C), F32)),
        in_specs=[any_space] * 2 + [vmem] * 3,
        out_specs=(vmem, vmem, any_space),
        scratch_shapes=scratch,
        compiler_params=pltpu.CompilerParams(collective_id=0, has_side_effects=True, vmem_limit_bytes=67_043_328),
    )(x, dy, *weights)


def adamw(w, m, v, g):
    m = 0.9 * m + 0.1 * g
    v = 0.95 * v + 0.05 * g * g
    step = m * lax.rsqrt(v + 1e-8) + 0.1 * w
    return (w - 0.02 * step).astype(BF16), m, v


def update(g, squares, *refs):
    ins, outs, held, (places, came, in_sem, out_sem) = refs[:9], refs[9:18], refs[18:27], refs[27:]
    copies = [pltpu.make_async_copy(a, b, in_sem.at[n]) for n, (a, b) in enumerate(zip(ins, held))]
    puts = [pltpu.make_async_copy(b, a, out_sem.at[n]) for n, (a, b) in enumerate(zip(outs, held))]
    for copy in copies:
        copy.start()
    for k in range(NK):
        places[k * C : k * C + C] = placement(k)
    count = 3 * 2 * D * FF
    factor = jnp.minimum(1.0, 0.5 * lax.rsqrt(jnp.sum(squares[...], keepdims=True) / count + 1e-30))
    chunks = [
        jnp.concatenate([g[NK + k, GATE], g[NK + k, UP], g[k, GATE], g[k, UP]]) for k in range(NK)
    ]
    came[...] = dot(jnp.concatenate(chunks, 1), places[...])
    for n in range(3):
        for which in range(n, 9, 3):
            copies[which].wait()
        w, m, v = held[n::3]
        step = SH // 2
        for layer in range(2):
            for row in range(0, w.shape[1], step):
                rows = slice(row, row + step)
                if n < 2:
                    first = (layer * 2 + n) * 64 + row
                    part = came[first : first + step]
                else:
                    q, inside = (1 - layer) * NK + row // SH, row % SH
                    part = jnp.concatenate(
                        [g[q, one.start + inside : one.start + inside + step] for one in (LOW, HIGH)], 1
                    ).astype(F32)
                w[layer, rows], m[layer, rows], v[layer, rows] = adamw(
                    w[layer, rows].astype(F32), m[layer, rows], v[layer, rows], part * factor
                )
        for which in range(n, 9, 3):
            puts[which].start()
    for put in puts:
        put.wait()


def updated(g, squares, arrays):
    any_space, vmem = pl.BlockSpec(memory_space=pl.ANY), pl.BlockSpec(memory_space=pltpu.VMEM)
    like = [jax.ShapeDtypeStruct(a.shape, a.dtype) for a in arrays]
    return pl.pallas_call(
        update,
        out_shape=like,
        in_specs=[vmem] * 2 + [any_space] * 9,
        out_specs=[any_space] * 9,
        scratch_shapes=[pltpu.VMEM(a.shape, a.dtype) for a in arrays]
        + [
            pltpu.VMEM((NK * C, FF), BF16),
            pltpu.VMEM((4 * 64, FF), F32),
            pltpu.SemaphoreType.DMA((9,)),
            pltpu.SemaphoreType.DMA((9,)),
        ],
        compiler_params=pltpu.CompilerParams(vmem_limit_bytes=60_000_000),
    )(g, squares, *arrays)


def solution(mesh):
    def step(x, dy, *arrays):
        g, squares, _ = gradients_of(x[0], dy[0], *arrays[:3])
        return tuple(updated(g, squares, arrays))

    states, cut = P(("rep", "dp"), None, None), P(None, "dp", None)
    return jax.shard_map(
        step,
        mesh=mesh,
        in_specs=(states, states) + (cut,) * 9,
        out_specs=(P("rep", "dp", None),) * 9,
        check_vma=False,
    )
```
